512 devices in a mesh: vocab: 64 (over y, x, core), grp: 8 (over z).
Axes of the slice: x: 4, y: 8, z: 8, core: 2. Of those that a mesh axis runs over, the one named last changes fastest.
Arguments:
- hidden: bfloat16 [2048, 4096], P('grp'), may hold values from -240 to 240
- head_weight: bfloat16 [4096, 32768], P('grp', 'vocab'), may hold values from -0.25 to 0.25
- cluster_weight: bfloat16 [4096, 3], replicated, may hold values from -0.5 to 0.5
- proj_one: bfloat16 [4096, 1024], P('vocab'), may hold values from -0.09375 to 0.09375
- proj_two: bfloat16 [4096, 256], P('vocab'), may hold values from -0.09375 to 0.09375
- proj_three: bfloat16 [4096, 64], P('vocab'), may hold values from -0.09375 to 0.09375
- tail_one: bfloat16 [1024, 65536], P('grp', 'vocab'), may hold values from -0.5 to 0.5
- tail_two: bfloat16 [256, 65536], P('grp', 'vocab'), may hold values from -1 to 1
- tail_three: bfloat16 [64, 65536], P('grp', 'vocab'), may hold values from -2 to 2
- targets: int32 [2048], P('grp'), may hold values from 0 to 229375, as said below
- flags: int32 [2048, 3], P('grp'), may hold values from 0 to 1, as said below
Outputs:
- target_logprob: float32 [2048], P('grp')
- tail_entropy: float32 [2048, 3], P('grp')
The draws below stay inside these ranges and needn't reach their ends.
Inputs may be any that keep to these rules, and one draw needn't show every extreme that they name: `targets`: a target at or beyond 32768 lies in tail (t - 32768) // 65536. flags[b, c] is 1 whenever the target of sequence b lies in tail c.
All inputs are finite; a program needn't handle non-finite values.
Results may differ from the reference program's by a relative error of at most 0.0092.
Values may be sent and summed in bfloat16 or wider, within the bound.
No kernel may reach another device: no remote copies, remote signals or barrier semaphores. Data moves between devices by JAX's collectives and lax.ppermute only.
A program may use at most 64 MiB of HBM per device.

```python
import jax
import jax.numpy as jnp
from jax import lax

D = 4096
V_HEAD = 32768
TAIL = 65536
P1 = 1024
P2 = 256
P3 = 64
ROWS_GRP = 256
BATCH_SEQUENCES = 2048


def draw_hidden(key, part):
    norm_random_key = jax.random.fold_in(jax.random.fold_in(key, 5), 0)
    values = jnp.clip(jax.random.normal(norm_random_key, (BATCH_SEQUENCES, D), jnp.float32), -6.0, 6.0)
    return values.astype(jnp.bfloat16)


def target_plan(key):
    base = jax.random.fold_in(key, 31)
    kkind, khead, ktail, kextra = jax.random.split(base, 4)
    kind = jax.random.randint(kkind, (BATCH_SEQUENCES,), 0, 5)
    head_word = jax.random.randint(khead, (BATCH_SEQUENCES,), 0, V_HEAD)
    tail_word = jax.random.randint(ktail, (BATCH_SEQUENCES,), 0, TAIL)
    chosen = jnp.where(kind < 2, head_word, V_HEAD + (kind - 2) * TAIL + tail_word).astype(jnp.int32)
    extra = jax.random.randint(kextra, (BATCH_SEQUENCES, 3), 0, 2)
    owned = (kind[:, None] - 2 == jnp.arange(3)[None, :]).astype(jnp.int32)
    return (chosen, jnp.maximum(extra, owned).astype(jnp.int32))


def draw_targets(key, part):
    return target_plan(key)[0]


def draw_flags(key, part):
    return target_plan(key)[1]


def steps_of(key, extent, cuts, smallest, high):
    def one(dim, blocks):
        heights = jax.random.uniform(jax.random.fold_in(jax.random.fold_in(key, 6), dim), (blocks,), jnp.float32, smallest / len(cuts), high / len(cuts))
        return jnp.repeat(jnp.exp(heights), extent[dim] // blocks).reshape((-1,) + (1,) * (len(extent) - dim - 1))

    level = one(*cuts[0])
    for cut in cuts[1:]:
        level = level * one(*cut)
    return level


def normal_values(key, dims, width, most, cuts=(), held_as=jnp.bfloat16):
    level = steps_of(key, dims, cuts, -0.22, 0.18) if cuts else 1.0
    entries = jax.random.normal(key, dims, jnp.float32) * width * level
    return jnp.minimum(jnp.maximum(entries, -most), most).astype(held_as)


def setup_inputs(seed: int = 0) -> dict:
    key_list = jax.random.split(jax.random.key(seed), 12)
    return {
        "hidden": draw_hidden(jax.random.fold_in(key_list[11], 71), 0),
        "head_weight": normal_values(key_list[1], (D, V_HEAD), (D // 9) ** -0.5, 0.25, ((0, 8), (1, 64))),
        "cluster_weight": normal_values(key_list[2], (D, 3), (D // 36) ** -0.5, 0.5),
        "proj_one": normal_values(key_list[3], (D, P1), D ** -0.5, 0.09375, ((0, 64),)),
        "proj_two": normal_values(key_list[4], (D, P2), D ** -0.5, 0.09375, ((0, 64),)),
        "proj_three": normal_values(key_list[5], (D, P3), D ** -0.5, 0.09375, ((0, 64),)),
        "tail_one": normal_values(key_list[6], (P1, TAIL), (P1 // 9) ** -0.5, 0.5, ((0, 8), (1, 64))),
        "tail_two": normal_values(key_list[7], (P2, TAIL), (P2 // 9) ** -0.5, 1.0, ((0, 8), (1, 64))),
        "tail_three": normal_values(key_list[8], (P3, TAIL), (max(P3 // 9, 1)) ** -0.5, 2.0, ((0, 8), (1, 64))),
        "targets": draw_targets(jax.random.fold_in(key_list[11], 71), 0),
        "flags": draw_flags(jax.random.fold_in(key_list[11], 71), 0),
    }


def tail_stats(projected, tail_weight):
    logits = jnp.dot(projected, tail_weight, preferred_element_type=jnp.float32)
    top = jnp.max(logits, axis=1)
    expo = jnp.exp(logits - top[:, None])
    total = jnp.sum(expo, axis=1)
    lse = top + jnp.log(total)
    mean = jnp.sum(expo * logits, axis=1) / total
    return logits, lse, mean


def reference(hidden, head_weight, cluster_weight, proj_one, proj_two, proj_three, tail_one, tail_two, tail_three, targets, flags):
    blocks = BATCH_SEQUENCES // ROWS_GRP
    hid_blocks = hidden.reshape(blocks, ROWS_GRP, D)
    tgt_blocks = targets.reshape(blocks, ROWS_GRP)
    flag_blocks = flags.reshape(blocks, ROWS_GRP, 3)
    projections = (proj_one, proj_two, proj_three)
    tails = (tail_one, tail_two, tail_three)

    def one_block(items):
        rows, tgt, flg = items
        head_logits = jnp.dot(rows, head_weight, preferred_element_type=jnp.float32)
        cluster_score_logits = jnp.dot(rows, cluster_weight, preferred_element_type=jnp.float32)
        top = jnp.maximum(jnp.max(head_logits, axis=1), jnp.max(cluster_score_logits, axis=1))
        total = jnp.sum(jnp.exp(head_logits - top[:, None]), axis=1) + jnp.sum(jnp.exp(cluster_score_logits - top[:, None]), axis=1)
        head_lse = top + jnp.log(total)
        relative = tgt - V_HEAD
        cluster = relative // TAIL
        word = relative - cluster * TAIL
        head_pick = jnp.take_along_axis(head_logits, jnp.clip(tgt, 0, V_HEAD - 1).astype(jnp.int32)[:, None], axis=1)[:, 0]
        lse_list = []
        mean_list = []
        tail_pick = jnp.zeros(tgt.shape, jnp.float32)
        for index in range(3):
            projected = jnp.dot(rows, projections[index], preferred_element_type=jnp.float32).astype(jnp.bfloat16)
            logits, lse, mean = tail_stats(projected, tails[index])
            lse_list.append(lse)
            mean_list.append(mean)
            picked = jnp.take_along_axis(logits, jnp.clip(word, 0, TAIL - 1).astype(jnp.int32)[:, None], axis=1)[:, 0]
            tail_pick = tail_pick + jnp.where(cluster == index, picked - lse + cluster_score_logits[:, index], 0.0)
        tail_lse = jnp.stack(lse_list, axis=1)
        tail_mean = jnp.stack(mean_list, axis=1)
        entropy = flg.astype(jnp.float32) * (tail_lse - tail_mean)
        logprob = jnp.where(tgt < V_HEAD, head_pick, tail_pick) - head_lse
        return logprob, entropy

    logprob, entropy = lax.map(one_block, (hid_blocks, tgt_blocks, flag_blocks))
    return logprob.reshape(BATCH_SEQUENCES), entropy.reshape(BATCH_SEQUENCES, 3)
```

```python
import functools

import jax
import jax.numpy as jnp
from jax import lax
from jax.experimental import pallas as pl
from jax.experimental.pallas import tpu as pltpu
from jax.sharding import Mesh
from jax.sharding import PartitionSpec as P

V_HEAD = 32768
TAIL = 65536
VOCAB = ("vocab_0", "vocab_1", "vocab_2")


def ring_gather(shard, axis):
    n = lax.axis_size(axis)
    up = [(i, (i + 1) % n) for i in range(n)]
    down = [(i, (i - 1) % n) for i in range(n)]
    found = {0: [shard]}
    right, left = shard, shard
    for step in range(1, n // 2):
        right = lax.ppermute(right, axis, up)
        left = lax.ppermute(left, axis, down)
        found[-step] = [right]
        found[step] = [left]
    half = shard.shape[0] // 2
    found[n // 2] = [lax.ppermute(right[:half], axis, up), lax.ppermute(left[half:], axis, down)]
    return found


def project_kernel(weight_ref, hidden_ref, out_ref):
    pairs = weight_ref.shape[0] // 2
    joined = jnp.concatenate(
        [
            jnp.concatenate([weight_ref[2 * k], weight_ref[2 * k + 1]], axis=1)
            for k in range(pairs)
        ],
        axis=1,
    )
    out_ref[...] = lax.dot_general(
        joined, hidden_ref[...], (((1,), (1,)), ((), ())), preferred_element_type=jnp.float32
    ).astype(out_ref.dtype)


def projected_share(weights, hidden):
    return pl.pallas_call(
        project_kernel,
        out_shape=jax.ShapeDtypeStruct((weights.shape[1], hidden.shape[0]), jnp.bfloat16),
        cost_estimate=pl.CostEstimate(
            flops=2 * weights.size * hidden.shape[0], bytes_accessed=3 << 20, transcendentals=0
        ),
    )(weights, hidden)


def copy_for_each(shard, axis):
    n = lax.psum(1, axis)
    copies = jnp.broadcast_to(shard, (n, *shard.shape))
    return lax.all_to_all(copies, axis, split_axis=0, concat_axis=0, tiled=True)


def combined(stats, axis):
    every = copy_for_each(stats, axis)
    tops = every[:, 0:4]
    top = jnp.max(tops, axis=0)
    scale = jnp.exp(tops - top)
    sums = jnp.sum(every[:, 4:8] * scale, axis=0)
    weighted = jnp.sum(every[:, 8:11] * scale[:, 1:4], axis=0)
    pick = jnp.sum(every[:, 11:12], axis=0)
    return jnp.concatenate([top, sums, weighted, pick], axis=0)


def shards(
    hidden,
    head_weight,
    cluster_weight,
    proj_one,
    proj_two,
    proj_three,
    tail_one,
    tail_two,
    tail_three,
    targets,
    flags,
):
    rows = hidden.shape[0]
    head_rows, head_cols = head_weight.shape
    tail_cols = tail_one.shape[1]
    half = tail_cols // 2
    n_vocab = lax.psum(1, VOCAB)
    n_grp = lax.axis_size("grp")
    vocab_index = lax.axis_index(VOCAB)
    grp_index = lax.axis_index("grp")

    widths = (proj_one.shape[1], proj_two.shape[1], proj_three.shape[1])
    total = sum(widths)
    share = -(-total // n_vocab // 8) * 8
    turned = jnp.concatenate((proj_one, proj_two, proj_three), axis=1).T
    turned = jnp.pad(turned, ((0, share * n_vocab - total), (0, 0)))
    pieces = turned.reshape(n_vocab, share, turned.shape[1])
    pieces = lax.all_to_all(pieces, VOCAB, split_axis=0, concat_axis=0, tiled=True)
    mine = projected_share(pieces, hidden)
    projected = copy_for_each(mine, VOCAB).reshape(n_vocab * share, rows)

    tails = (tail_one, tail_two, tail_three)
    packed = jnp.concatenate(
        [part for tail in tails for part in (tail[:, :half], tail[:, half:])], axis=0
    )
    tail_found = ring_gather(packed, "grp")
    head_found = ring_gather(head_weight, "grp")

    full = [jnp.zeros((2, tail.shape[0] * n_grp, half), tail.dtype) for tail in tails]
    for offset, parts in tail_found.items():
        block = parts[0] if len(parts) == 1 else jnp.concatenate(parts, axis=0)
        owner = (grp_index + offset) % n_grp
        at = 0
        for k, tail in enumerate(tails):
            height = tail.shape[0]
            both = block[at : at + 2 * height].reshape(2, height, half)
            full[k] = lax.dynamic_update_slice(full[k], both, (0, owner * height, 0))
            at += 2 * height
    at = 0
    tail_logits = []
    for k, width in enumerate(widths):
        tail_logits.append(
            jnp.concatenate(
                [
                    lax.dot_general(
                        projected[at : at + width],
                        full[k][side],
                        (((0,), (0,)), ((), ())),
                        preferred_element_type=jnp.float32,
                    )
                    for side in range(2)
                ],
                axis=1,
            )
        )
        at += width

    head_logits = None
    for offset, parts in head_found.items():
        owner = (grp_index + offset) % n_grp
        at = 0
        for part in parts:
            features = lax.dynamic_slice_in_dim(
                hidden, owner * head_rows + at, part.shape[0], 1
            )
            term = jnp.dot(features, part, preferred_element_type=jnp.float32)
            head_logits = term if head_logits is None else head_logits + term
            at += part.shape[0]

    cluster_logits = jnp.dot(hidden, cluster_weight, preferred_element_type=jnp.float32)

    relative = targets - V_HEAD
    cluster = relative // TAIL
    word = relative - cluster * TAIL
    tail_ids = vocab_index * tail_cols + jnp.arange(tail_cols, dtype=jnp.int32)
    same_word = tail_ids[None, :] == word[:, None]
    tail_pick = jnp.zeros((rows,), jnp.float32)
    tops, sums, weighted = [], [], []
    for k in range(3):
        logits = tail_logits[k]
        hit = jnp.logical_and(same_word, (cluster == k)[:, None])
        tail_pick = tail_pick + jnp.sum(jnp.where(hit, logits, 0.0), axis=1)
        top = jnp.max(logits, axis=1)
        expo = jnp.exp(logits - top[:, None])
        tops.append(top)
        sums.append(jnp.sum(expo, axis=1))
        weighted.append(jnp.sum(expo * logits, axis=1))
    head_ids = vocab_index * head_cols + jnp.arange(head_cols, dtype=jnp.int32)
    head_pick = jnp.sum(jnp.where(head_ids[None, :] == targets[:, None], head_logits, 0.0), axis=1)
    head_top = jnp.max(head_logits, axis=1)
    head_sum = jnp.sum(jnp.exp(head_logits - head_top[:, None]), axis=1)
    stats = jnp.stack(
        [head_top, *tops, head_sum, *sums, *weighted, head_pick + tail_pick], axis=0
    )
    stats = combined(stats, VOCAB[1:])
    stats = combined(stats, VOCAB[:1])

    scores = cluster_logits.T
    top = jnp.maximum(stats[0], jnp.max(scores, axis=0))
    all_sum = stats[4] * jnp.exp(stats[0] - top) + jnp.sum(jnp.exp(scores - top), axis=0)
    head_lse = top + jnp.log(all_sum)
    tail_sum = stats[5:8]
    tail_lse = stats[1:4] + jnp.log(tail_sum)
    tail_mean = stats[8:11] / tail_sum
    entropy = flags.T.astype(jnp.float32) * (tail_lse - tail_mean)
    which = cluster[None, :] == jnp.arange(3, dtype=jnp.int32)[:, None]
    cluster_term = jnp.sum(jnp.where(which, scores - tail_lse, 0.0), axis=0)
    picked = stats[11]
    target_logprob = jnp.where(targets < V_HEAD, picked, picked + cluster_term) - head_lse
    return (target_logprob, entropy.T)


def solution(mesh):
    finer = Mesh(
        mesh.devices.reshape(8, 4, 2, mesh.shape["grp"]), ("vocab_0", "vocab_1", "vocab_2", "grp")
    )
    in_specs = (
        P("grp", None),
        P("grp", VOCAB),
        P(),
        P(VOCAB, None),
        P(VOCAB, None),
        P(VOCAB, None),
        P("grp", VOCAB),
        P("grp", VOCAB),
        P("grp", VOCAB),
        P("grp"),
        P("grp", None),
    )
    out_specs = (P("grp"), P("grp", None))
    return jax.shard_map(
        shards, mesh=finer, in_specs=in_specs, out_specs=out_specs, check_vma=False
    )
```

```python
import functools

import jax
import jax.numpy as jnp
from jax import lax
from jax.experimental import pallas as pl
from jax.experimental.pallas import tpu as pltpu
from jax.sharding import Mesh
from jax.sharding import PartitionSpec as P


V_HEAD = 32768
TAIL = 65536
VOCAB = ("vocab_0", "vocab_1", "vocab_2")
CHIPS, CORE = VOCAB[:2], VOCAB[2]


def ring(shard, axis, cut):
    n = lax.axis_size(axis)
    up = [(i, (i + 1) % n) for i in range(n)]
    down = [(i, (i - 1) % n) for i in range(n)]
    found = {}
    right, left = shard, shard
    for step in range(1, n // 2):
        right = lax.ppermute(right, axis, up)
        left = lax.ppermute(left, axis, down)
        found[-step], found[step] = right, left
    first = lax.ppermute(right[:cut], axis, up)
    second = lax.ppermute(left[cut:], axis, down)
    return found, first, second


def copy_for_each(shard, axis):
    n = lax.psum(1, axis)
    copies = jnp.broadcast_to(shard, (n, *shard.shape))
    return lax.all_to_all(copies, axis, split_axis=0, concat_axis=0, tiled=True)


def dot(a, b):
    return jnp.dot(a, b, preferred_element_type=jnp.float32)


def kernel_call(body, out_shape, flops, scratch=(), mib=16):
    vmem = pl.BlockSpec(memory_space=pltpu.VMEM)
    smem = pl.BlockSpec(memory_space=pltpu.SMEM)

    def call(scalars, *arrays):
        return pl.pallas_call(
            body,
            out_shape=out_shape,
            in_specs=[smem] * (scalars is not None) + [vmem] * len(arrays),
            out_specs=jax.tree.map(lambda _: vmem, out_shape),
            scratch_shapes=list(scratch),
            cost_estimate=pl.CostEstimate(flops=flops, bytes_accessed=1 << 20, transcendentals=0),
            compiler_params=pltpu.CompilerParams(vmem_limit_bytes=mib << 20),
        )(*(() if scalars is None else (scalars,)), *arrays)

    return call


def project_kernel(weight_ref, hidden_ref, out_ref):
    joined = jnp.concatenate([weight_ref[k] for k in range(weight_ref.shape[0])], axis=1)
    out_ref[...] = lax.dot_general(
        joined, hidden_ref[...], (((1,), (1,)), ((), ())), preferred_element_type=jnp.float32
    ).astype(out_ref.dtype)


def spread(block, owner, count):
    tall = jnp.concatenate([block] * count, axis=0)
    row = lax.broadcasted_iota(jnp.int32, tall.shape, 0)
    return tall, row // block.shape[0] == owner


def part_kernel(h, owner_ref, turned_ref, hidden_ref, *refs):
    shard_refs = refs[: h.count - 1]
    proj_ref, head_ref, one_ref, two_ref, three_ref, wide_ref = refs[h.count - 1 :]
    proj_ref[...] = turned_ref[...].T
    n, half = h.count, h.half
    last = owner_ref[n - 1]
    blank = jnp.zeros((h.one, half), wide_ref.dtype)
    small = jnp.zeros((h.two, half), wide_ref.dtype)
    for side in range(2):
        wide_ref[side, pl.ds(pl.multiple_of(last * h.one, h.one), h.one), :] = blank
        two_ref[side, pl.ds(pl.multiple_of(last * h.two, h.two), h.two), :] = small
    threes = [jnp.zeros((h.three * n, half), jnp.float32)] * 2
    head = None
    for k, ref in enumerate(shard_refs):
        owner = owner_ref[k]
        for side in range(2):
            wide_ref[side, pl.ds(pl.multiple_of(owner * h.one, h.one), h.one), :] = ref[
                side * h.one : (side + 1) * h.one, :
            ]
            at = 2 * h.one + side * h.two
            two_ref[side, pl.ds(pl.multiple_of(owner * h.two, h.two), h.two), :] = ref[
                at : at + h.two, :
            ]
        both = ref[h.three_at : h.head_at, :].astype(jnp.float32)
        for side in range(2):
            tall, there = spread(both[side * h.three : (side + 1) * h.three], owner, n)
            threes[side] = jnp.where(there, tall, threes[side])
        features = hidden_ref[:, pl.ds(pl.multiple_of(owner * h.head, h.head), h.head)]
        term = dot(features, ref[h.head_at :, :])
        head = term if head is None else head + term
    head_ref[...] = head
    for side in range(2):
        three_ref[side] = threes[side].astype(three_ref.dtype)
        one_ref[:, side * half : (side + 1) * half] = dot(
            proj_ref[:, : h.one * n], wide_ref[side]
        )


def last_kernel(
    h,
    owner_ref,
    first_ref,
    second_ref,
    hidden_ref,
    proj_ref,
    head_ref,
    one_ref,
    two_ref,
    three_ref,
    ids_ref,
    out_ref,
    wide_ref,
):
    n, half = h.count, h.half
    owner = owner_ref[n - 1]
    rows = hidden_ref.shape[0]
    rest = h.cut - h.head_at
    at = pl.multiple_of(owner * h.head, h.head)
    head = head_ref[...] + dot(hidden_ref[:, pl.ds(at, rest)], first_ref[h.head_at :, :])
    at = pl.multiple_of(owner * h.head + rest, 128)
    head = head + dot(hidden_ref[:, pl.ds(at, h.head - rest)], second_ref[...])
    one_features = proj_ref[:, pl.ds(pl.multiple_of(owner * h.one, h.one), h.one)]
    two_features = proj_ref[:, h.one * n : (h.one + h.two) * n]
    three_features = proj_ref[:, (h.one + h.two) * n : (h.one + h.two + h.three) * n]
    wide_ref[...] = two_ref[...]
    both = first_ref[h.three_at : h.head_at, :].astype(jnp.float32)
    ones, twos, threes = [], [], []
    for side in range(2):
        ones.append(
            one_ref[:, side * half : (side + 1) * half]
            + dot(one_features, first_ref[side * h.one : (side + 1) * h.one, :])
        )
        at = 2 * h.one + side * h.two
        wide_ref[side, pl.ds(pl.multiple_of(owner * h.two, h.two), h.two), :] = first_ref[
            at : at + h.two, :
        ]
        twos.append(dot(two_features, wide_ref[side]))
        tall, there = spread(both[side * h.three : (side + 1) * h.three], owner, n)
        block = jnp.where(there, tall, three_ref[side].astype(jnp.float32))
        threes.append(dot(three_features, block.astype(three_ref.dtype)))
    columns = []
    pick = jnp.zeros((rows, 1), jnp.float32)
    tops, sums, weighted = [], [], []
    for k, sides in enumerate(([head], ones, twos, threes)):
        top = functools.reduce(
            jnp.maximum, [jnp.max(logits, axis=1, keepdims=True) for logits in sides]
        )
        total = jnp.zeros((rows, 1), jnp.float32)
        mass = jnp.zeros((rows, 1), jnp.float32)
        for side, logits in enumerate(sides):
            expo = jnp.exp(logits - top)
            total = total + jnp.sum(expo, axis=1, keepdims=True)
            if k:
                mass = mass + jnp.sum(expo * logits, axis=1, keepdims=True)
            word = lax.broadcasted_iota(jnp.int32, logits.shape, 1) + side * half
            hit = word == ids_ref[:, k : k + 1]
            pick = pick + jnp.sum(jnp.where(hit, logits, 0.0), axis=1, keepdims=True)
        tops.append(top)
        sums.append(total)
        if k:
            weighted.append(mass)
    columns = [*tops, *sums, *weighted, pick]
    lane = lax.broadcasted_iota(jnp.int32, (rows, 128), 1)
    table = jnp.zeros((rows, 128), jnp.float32)
    for k, column in enumerate(columns):
        table = jnp.where(lane == k, column, table)
    out_ref[...] = table.T[: out_ref.shape[0]]


def combined(every):
    tops = every[:, 0:4]
    top = jnp.max(tops, axis=0)
    scale = jnp.exp(tops - top)
    sums = jnp.sum(every[:, 4:8] * scale, axis=0)
    weighted = jnp.sum(every[:, 8:11] * scale[:, 1:4], axis=0)
    pick = jnp.sum(every[:, 11:12], axis=0)
    return jnp.concatenate([top, sums, weighted, pick], axis=0)


class Heights:
    def __init__(self, count, one, two, three, head, half):
        self.count, self.one, self.two, self.three = count, one, two, three
        self.head, self.half = head, half
        self.three_at = 2 * (one + two)
        self.head_at = 2 * (one + two + three)
        self.cut = self.head_at + 128


def one_device(
    hidden,
    head_weight,
    cluster_weight,
    proj_one,
    proj_two,
    proj_three,
    tail_one,
    tail_two,
    tail_three,
    targets,
    flags,
):
    rows = hidden.shape[0]
    head_cols = head_weight.shape[1]
    tail_cols = tail_one.shape[1]
    half = tail_cols // 2
    n_chips = lax.psum(1, CHIPS)
    n_grp = lax.axis_size("grp")
    core = lax.axis_index(CORE)
    vocab_index = lax.axis_index(VOCAB)
    grp_index = lax.axis_index("grp")

    tails = (tail_one, tail_two, tail_three)
    h = Heights(n_grp, *(t.shape[0] for t in tails), head_weight.shape[0], half)
    packed = jnp.concatenate(
        [part for tail in tails for part in (tail[:, :half], tail[:, half:])] + [head_weight], axis=0
    )
    found, first, second = ring(packed, "grp", h.cut)
    offsets = [0, *found, n_grp // 2]
    owners = (grp_index + jnp.array(offsets, jnp.int32)) % n_grp

    widths = (proj_one.shape[1], proj_two.shape[1], proj_three.shape[1])
    total = sum(widths)
    share = -(-total // (2 * n_chips) // 8) * 8
    joined = lax.all_gather(
        jnp.concatenate((proj_one, proj_two, proj_three), axis=1), CORE, axis=0, tiled=True
    )
    turned = jnp.pad(joined.T, ((0, 2 * n_chips * share - total), (0, 0)))
    turned = turned.reshape(2, n_chips, share, joined.shape[0])
    pieces = lax.dynamic_index_in_dim(turned, core, 0, keepdims=False)
    pieces = lax.all_to_all(pieces, CHIPS, split_axis=0, concat_axis=0, tiled=True)
    mine = kernel_call(
        project_kernel,
        jax.ShapeDtypeStruct((share, rows), jnp.bfloat16),
        2 * share * hidden.size,
    )(None, pieces, hidden)
    turned = copy_for_each(mine, CHIPS)
    turned = lax.all_gather(turned, CORE)
    turned = turned.reshape(2 * n_chips * share, rows)

    wide = jnp.bfloat16
    part_call = kernel_call(
        functools.partial(part_kernel, h),
        (
            jax.ShapeDtypeStruct((rows, turned.shape[0]), wide),
            jax.ShapeDtypeStruct((rows, head_cols), jnp.float32),
            jax.ShapeDtypeStruct((rows, tail_cols), jnp.float32),
            jax.ShapeDtypeStruct((2, h.two * n_grp, half), wide),
            jax.ShapeDtypeStruct((2, h.three * n_grp, half), wide),
        ),
        2 * rows * packed.size * n_grp,
        [pltpu.VMEM((2, h.one * n_grp, half), wide)],
    )
    part = part_call(owners, turned, hidden, packed, *found.values())

    cluster_logits = dot(hidden, cluster_weight)
    relative = targets - V_HEAD
    cluster = relative // TAIL
    word = relative - cluster * TAIL
    ids = jnp.stack(
        [targets - vocab_index * head_cols]
        + [jnp.where(cluster == k, word - vocab_index * tail_cols, -1) for k in range(3)],
        axis=1,
    )
    stats = kernel_call(
        functools.partial(last_kernel, h),
        jax.ShapeDtypeStruct((12, rows), jnp.float32),
        2 * rows * packed.size,
        [pltpu.VMEM((2, h.two * n_grp, half), wide)],
    )(owners, first, second, hidden, *part, ids)

    mid = rows // 2

    def own(array):
        return lax.dynamic_slice_in_dim(array, core * mid, mid, array.ndim - 1)

    stats = combined(own(lax.all_gather(stats, CORE)))
    stats = combined(copy_for_each(stats, CHIPS))
    scores, cluster, targets = own(cluster_logits.T), own(cluster), own(targets)
    top = jnp.maximum(stats[0], jnp.max(scores, axis=0))
    all_sum = stats[4] * jnp.exp(stats[0] - top) + jnp.sum(jnp.exp(scores - top), axis=0)
    head_lse = top + jnp.log(all_sum)
    tail_sum = stats[5:8]
    tail_lse = stats[1:4] + jnp.log(tail_sum)
    tail_mean = stats[8:11] / tail_sum
    entropy = own(flags.T).astype(jnp.float32) * (tail_lse - tail_mean)
    which = cluster[None, :] == jnp.arange(3, dtype=jnp.int32)[:, None]
    cluster_term = jnp.sum(jnp.where(which, scores - tail_lse, 0.0), axis=0)
    picked = stats[11]
    target_logprob = jnp.where(targets < V_HEAD, picked, picked + cluster_term) - head_lse
    final = lax.all_gather(
        jnp.concatenate([target_logprob[None], entropy], axis=0), CORE, axis=1, tiled=True
    )
    return (final[0], final[1:].T)


def solution(mesh):
    finer = Mesh(
        mesh.devices.reshape(8, 4, 2, mesh.shape["grp"]), ("vocab_0", "vocab_1", "vocab_2", "grp")
    )
    in_specs = (
        P("grp", None),
        P("grp", VOCAB),
        P(),
        P(VOCAB, None),
        P(VOCAB, None),
        P(VOCAB, None),
        P("grp", VOCAB),
        P("grp", VOCAB),
        P("grp", VOCAB),
        P("grp"),
        P("grp", None),
    )
    out_specs = (P("grp"), P("grp", None))
    return jax.shard_map(
        one_device, mesh=finer, in_specs=in_specs, out_specs=out_specs, check_vma=False
    )
```

```python
import functools

import jax
import jax.numpy as jnp
from jax import lax
from jax.experimental import pallas as pl
from jax.experimental.pallas import tpu as pltpu
from jax.sharding import Mesh
from jax.sharding import PartitionSpec as P


V_HEAD = 32768
TAIL = 65536
VOCAB = ("vocab_0", "vocab_1", "vocab_2")
CHIPS, CORE = VOCAB[:2], VOCAB[2]


def ring(shard, axis, cut):
    n = lax.axis_size(axis)
    up = [(i, (i + 1) % n) for i in range(n)]
    down = [(i, (i - 1) % n) for i in range(n)]
    found = {}
    right, left = shard, shard
    for step in range(1, n // 2):
        right = lax.ppermute(right, axis, up)
        left = lax.ppermute(left, axis, down)
        found[-step], found[step] = right, left
    first = lax.ppermute(right[:cut], axis, up)
    second = lax.ppermute(left[cut:], axis, down)
    return found, first, second


def copy_for_each(shard, axis):
    n = lax.psum(1, axis)
    copies = jnp.broadcast_to(shard, (n, *shard.shape))
    return lax.all_to_all(copies, axis, split_axis=0, concat_axis=0, tiled=True)


def dot(a, b):
    return jnp.dot(a, b, preferred_element_type=jnp.float32)


def kernel_call(body, out_shape, flops, scratch=(), mib=16):
    vmem = pl.BlockSpec(memory_space=pltpu.VMEM)
    smem = pl.BlockSpec(memory_space=pltpu.SMEM)

    def call(scalars, *arrays):
        return pl.pallas_call(
            body,
            out_shape=out_shape,
            in_specs=[smem] * (scalars is not None) + [vmem] * len(arrays),
            out_specs=jax.tree.map(lambda _: vmem, out_shape),
            scratch_shapes=list(scratch),
            cost_estimate=pl.CostEstimate(flops=flops, bytes_accessed=1 << 20, transcendentals=0),
            compiler_params=pltpu.CompilerParams(vmem_limit_bytes=mib << 20),
        )(*(() if scalars is None else (scalars,)), *arrays)

    return call


def pack_kernel(places, *refs):
    sources, out_ref, sems = refs[:-2], refs[-2], refs[-1]
    copies = []
    for k, (source, left, at) in enumerate(places):
        ref = sources[source]
        copies.append(
            pltpu.make_async_copy(
                ref.at[:, pl.ds(left, out_ref.shape[1])],
                out_ref.at[pl.ds(at, ref.shape[0]), :],
                sems.at[k],
            )
        )
    for copy in copies:
        copy.start()
    for copy in copies:
        copy.wait()


def packed_rows(sources, width):
    places, at = [], 0
    for k, source in enumerate(sources):
        for left in range(0, source.shape[1], width):
            places.append((k, left, at))
            at += source.shape[0]
    return pl.pallas_call(
        functools.partial(pack_kernel, places),
        out_shape=jax.ShapeDtypeStruct((at, width), sources[0].dtype),
        in_specs=[pl.BlockSpec(memory_space=pltpu.HBM)] * len(sources),
        out_specs=pl.BlockSpec(memory_space=pltpu.VMEM),
        scratch_shapes=[pltpu.SemaphoreType.DMA((len(places),))],
    )(*sources)


def project_kernel(weight_ref, hidden_ref, out_ref):
    joined = jnp.concatenate([weight_ref[k] for k in range(weight_ref.shape[0])], axis=1)
    out_ref[...] = lax.dot_general(
        joined, hidden_ref[...], (((1,), (1,)), ((), ())), preferred_element_type=jnp.float32
    ).astype(out_ref.dtype)


def spread(block, owner, count):
    tall = jnp.concatenate([block] * count, axis=0)
    row = lax.broadcasted_iota(jnp.int32, tall.shape, 0)
    return tall, row // block.shape[0] == owner


def part_kernel(h, owner_ref, turned_ref, hidden_ref, *refs):
    shard_refs = refs[: h.count - 1]
    proj_ref, head_ref, one_ref, two_ref, three_ref, wide_ref = refs[h.count - 1 :]
    proj_ref[...] = turned_ref[...].T
    n, half = h.count, h.half
    last = owner_ref[n - 1]
    blank = jnp.zeros((h.one, half), wide_ref.dtype)
    small = jnp.zeros((h.two, half), wide_ref.dtype)
    for side in range(2):
        wide_ref[side, pl.ds(pl.multiple_of(last * h.one, h.one), h.one), :] = blank
        two_ref[side, pl.ds(pl.multiple_of(last * h.two, h.two), h.two), :] = small
    threes = [jnp.zeros((h.three * n, half), jnp.float32)] * 2
    head = None
    for k, ref in enumerate(shard_refs):
        owner = owner_ref[k]
        for side in range(2):
            wide_ref[side, pl.ds(pl.multiple_of(owner * h.one, h.one), h.one), :] = ref[
                side * h.one : (side + 1) * h.one, :
            ]
            at = 2 * h.one + side * h.two
            two_ref[side, pl.ds(pl.multiple_of(owner * h.two, h.two), h.two), :] = ref[
                at : at + h.two, :
            ]
        both = ref[h.three_at : h.head_at, :].astype(jnp.float32)
        for side in range(2):
            tall, there = spread(both[side * h.three : (side + 1) * h.three], owner, n)
            threes[side] = jnp.where(there, tall, threes[side])
        features = hidden_ref[:, pl.ds(pl.multiple_of(owner * h.head, h.head), h.head)]
        term = dot(features, ref[h.head_at :, :])
        head = term if head is None else head + term
    head_ref[...] = head
    for side in range(2):
        three_ref[side] = threes[side].astype(three_ref.dtype)
        one_ref[:, side * half : (side + 1) * half] = dot(
            proj_ref[:, : h.one * n], wide_ref[side]
        )


def last_kernel(
    h,
    owner_ref,
    first_ref,
    second_ref,
    hidden_ref,
    proj_ref,
    head_ref,
    one_ref,
    two_ref,
    three_ref,
    ids_ref,
    out_ref,
    wide_ref,
):
    n, half = h.count, h.half
    owner = owner_ref[n - 1]
    rows = hidden_ref.shape[0]
    rest = h.cut - h.head_at
    at = pl.multiple_of(owner * h.head, h.head)
    head = head_ref[...] + dot(hidden_ref[:, pl.ds(at, rest)], first_ref[h.head_at :, :])
    at = pl.multiple_of(owner * h.head + rest, 128)
    head = head + dot(hidden_ref[:, pl.ds(at, h.head - rest)], second_ref[...])
    one_features = proj_ref[:, pl.ds(pl.multiple_of(owner * h.one, h.one), h.one)]
    two_features = proj_ref[:, h.one * n : (h.one + h.two) * n]
    three_features = proj_ref[:, (h.one + h.two) * n : (h.one + h.two + h.three) * n]
    wide_ref[...] = two_ref[...]
    both = first_ref[h.three_at : h.head_at, :].astype(jnp.float32)
    ones, twos, threes = [], [], []
    for side in range(2):
        ones.append(
            one_ref[:, side * half : (side + 1) * half]
            + dot(one_features, first_ref[side * h.one : (side + 1) * h.one, :])
        )
        at = 2 * h.one + side * h.two
        wide_ref[side, pl.ds(pl.multiple_of(owner * h.two, h.two), h.two), :] = first_ref[
            at : at + h.two, :
        ]
        twos.append(dot(two_features, wide_ref[side]))
        tall, there = spread(both[side * h.three : (side + 1) * h.three], owner, n)
        block = jnp.where(there, tall, three_ref[side].astype(jnp.float32))
        threes.append(dot(three_features, block.astype(three_ref.dtype)))
    columns = []
    pick = jnp.zeros((rows, 1), jnp.float32)
    tops, sums, weighted = [], [], []
    for k, sides in enumerate(([head], ones, twos, threes)):
        top = functools.reduce(
            jnp.maximum, [jnp.max(logits, axis=1, keepdims=True) for logits in sides]
        )
        total = jnp.zeros((rows, 1), jnp.float32)
        mass = jnp.zeros((rows, 1), jnp.float32)
        for side, logits in enumerate(sides):
            expo = jnp.exp(logits - top)
            total = total + jnp.sum(expo, axis=1, keepdims=True)
            if k:
                mass = mass + jnp.sum(expo * logits, axis=1, keepdims=True)
            word = lax.broadcasted_iota(jnp.int32, logits.shape, 1) + side * half
            hit = word == ids_ref[:, k : k + 1]
            pick = pick + jnp.sum(jnp.where(hit, logits, 0.0), axis=1, keepdims=True)
        tops.append(top)
        sums.append(total)
        if k:
            weighted.append(mass)
    columns = [*tops, *sums, *weighted, pick]
    lane = lax.broadcasted_iota(jnp.int32, (rows, 128), 1)
    table = jnp.zeros((rows, 128), jnp.float32)
    for k, column in enumerate(columns):
        table = jnp.where(lane == k, column, table)
    out_ref[...] = table.T[: out_ref.shape[0]]


def combined(rows, axis):
    def down(combine, array):
        return combine(array, axis=axis, keepdims=True)

    tops = [down(jnp.max, row) for row in rows[0:4]]
    scales = [jnp.exp(row - top) for row, top in zip(rows[0:4], tops)]
    sums = [down(jnp.sum, row * scale) for row, scale in zip(rows[4:8], scales)]
    masses = [down(jnp.sum, row * scale) for row, scale in zip(rows[8:11], scales[1:])]
    return [*tops, *sums, *masses, down(jnp.sum, rows[11])]


def merge_kernel(core_ref, stats_ref, out_ref):
    mid = stats_ref.shape[2] // 2
    lanes = pl.ds(pl.multiple_of(core_ref[0] * mid, mid), mid)
    both = [stats_ref[core, :, lanes] for core in range(2)]
    rows = [jnp.concatenate([table[k : k + 1] for table in both], axis=0) for k in range(12)]
    for k, row in enumerate(combined(rows, 0)):
        out_ref[:, 0, k * mid : (k + 1) * mid] = jnp.broadcast_to(row, (out_ref.shape[0], mid))


def finish_kernel(core_ref, stats_ref, scores_ref, flags_ref, targets_ref, out_ref):
    mid = out_ref.shape[1]
    lanes = pl.ds(pl.multiple_of(core_ref[0] * mid, mid), mid)
    rows = combined([stats_ref[:, 0, k * mid : (k + 1) * mid] for k in range(12)], 0)
    scores, flags = scores_ref[:, lanes], flags_ref[:, lanes]
    targets = targets_ref[:, lanes]
    top = jnp.maximum(rows[0], jnp.max(scores, axis=0, keepdims=True))
    total = rows[4] * jnp.exp(rows[0] - top) + jnp.sum(
        jnp.exp(scores - top), axis=0, keepdims=True
    )
    head_lse = top + jnp.log(total)
    picked = rows[11]
    for k in range(3):
        lse = rows[1 + k] + jnp.log(rows[5 + k])
        mean = rows[8 + k] / rows[5 + k]
        out_ref[1 + k : 2 + k, :] = flags[k : k + 1].astype(jnp.float32) * (lse - mean)
        low = V_HEAD + k * TAIL
        inside = jnp.logical_and(targets >= low, targets < low + TAIL)
        picked = picked + jnp.where(inside, scores[k : k + 1] - lse, 0.0)
    out_ref[0:1, :] = picked - head_lse


class Heights:
    def __init__(self, count, one, two, three, head, half):
        self.count, self.one, self.two, self.three = count, one, two, three
        self.head, self.half = head, half
        self.three_at = 2 * (one + two)
        self.head_at = 2 * (one + two + three)
        self.cut = self.head_at + 128


def one_device(
    hidden,
    head_weight,
    cluster_weight,
    proj_one,
    proj_two,
    proj_three,
    tail_one,
    tail_two,
    tail_three,
    targets,
    flags,
):
    rows = hidden.shape[0]
    head_cols = head_weight.shape[1]
    tail_cols = tail_one.shape[1]
    half = tail_cols // 2
    n_chips = lax.psum(1, CHIPS)
    n_grp = lax.axis_size("grp")
    core = lax.axis_index(CORE)
    vocab_index = lax.axis_index(VOCAB)
    grp_index = lax.axis_index("grp")

    tails = (tail_one, tail_two, tail_three)
    h = Heights(n_grp, *(t.shape[0] for t in tails), head_weight.shape[0], half)
    packed = packed_rows((*tails, head_weight), half)
    found, first, second = ring(packed, "grp", h.cut)
    offsets = [0, *found, n_grp // 2]
    owners = (grp_index + jnp.array(offsets, jnp.int32)) % n_grp

    widths = (proj_one.shape[1], proj_two.shape[1], proj_three.shape[1])
    total = sum(widths)
    share = -(-total // (2 * n_chips) // 8) * 8
    joined = lax.all_gather(
        jnp.concatenate((proj_one, proj_two, proj_three), axis=1), CORE, axis=0, tiled=True
    )
    turned = jnp.pad(joined.T, ((0, 2 * n_chips * share - total), (0, 0)))
    turned = turned.reshape(2, n_chips, share, joined.shape[0])
    pieces = lax.dynamic_index_in_dim(turned, core, 0, keepdims=False)
    pieces = lax.all_to_all(pieces, CHIPS, split_axis=0, concat_axis=0, tiled=True)
    mine = kernel_call(
        project_kernel,
        jax.ShapeDtypeStruct((share, rows), jnp.bfloat16),
        2 * share * hidden.size,
    )(None, pieces, hidden)
    turned = copy_for_each(mine, CHIPS)
    turned = lax.all_gather(turned, CORE)
    turned = turned.reshape(2 * n_chips * share, rows)

    wide = jnp.bfloat16
    part_call = kernel_call(
        functools.partial(part_kernel, h),
        (
            jax.ShapeDtypeStruct((rows, turned.shape[0]), wide),
            jax.ShapeDtypeStruct((rows, head_cols), jnp.float32),
            jax.ShapeDtypeStruct((rows, tail_cols), jnp.float32),
            jax.ShapeDtypeStruct((2, h.two * n_grp, half), wide),
            jax.ShapeDtypeStruct((2, h.three * n_grp, half), wide),
        ),
        2 * rows * packed.size * n_grp,
        [pltpu.VMEM((2, h.one * n_grp, half), wide)],
    )
    part = part_call(owners, turned, hidden, packed, *found.values())

    cluster_logits = dot(hidden, cluster_weight)
    relative = targets - V_HEAD
    cluster = relative // TAIL
    word = relative - cluster * TAIL
    ids = jnp.stack(
        [targets - vocab_index * head_cols]
        + [jnp.where(cluster == k, word - vocab_index * tail_cols, -1) for k in range(3)],
        axis=1,
    )
    stats = kernel_call(
        functools.partial(last_kernel, h),
        jax.ShapeDtypeStruct((12, rows), jnp.float32),
        2 * rows * packed.size,
        [pltpu.VMEM((2, h.two * n_grp, half), wide)],
    )(owners, first, second, hidden, *part, ids)

    mid = rows // 2
    which = jnp.reshape(core, (1,)).astype(jnp.int32)
    copies = kernel_call(
        merge_kernel, jax.ShapeDtypeStruct((n_chips, 1, 12 * mid), jnp.float32), 1 << 20, mib=4
    )(which, lax.all_gather(stats, CORE))
    copies = lax.all_to_all(copies, CHIPS, split_axis=0, concat_axis=0, tiled=True)
    final = kernel_call(
        finish_kernel, jax.ShapeDtypeStruct((4, mid), jnp.float32), 1 << 20, mib=4
    )(which, copies, cluster_logits.T, flags.T, targets[None])
    final = lax.all_gather(final, CORE, axis=1, tiled=True)
    return (final[0], final[1:].T)


def solution(mesh):
    finer = Mesh(
        mesh.devices.reshape(8, 4, 2, mesh.shape["grp"]), ("vocab_0", "vocab_1", "vocab_2", "grp")
    )
    in_specs = (
        P("grp", None),
        P("grp", VOCAB),
        P(),
        P(VOCAB, None),
        P(VOCAB, None),
        P(VOCAB, None),
        P("grp", VOCAB),
        P("grp", VOCAB),
        P("grp", VOCAB),
        P("grp"),
        P("grp", None),
    )
    out_specs = (P("grp"), P("grp", None))
    return jax.shard_map(
        one_device, mesh=finer, in_specs=in_specs, out_specs=out_specs, check_vma=False
    )
```

```python
import functools

import jax
import jax.numpy as jnp
from jax import lax
from jax.experimental import pallas as pl
from jax.experimental.pallas import tpu as pltpu
from jax.sharding import Mesh
from jax.sharding import PartitionSpec as P


V_HEAD = 32768
TAIL = 65536
VOCAB = ("vocab_0", "vocab_1", "vocab_2")
CHIPS, CORE = VOCAB[:2], VOCAB[2]


def ring(shard, axis, cut):
    n = lax.axis_size(axis)
    even = [(i, i ^ 1) for i in range(n)]
    odd = [(i, ((i + 1) ^ 1) - 1 if 0 < i < n - 1 else n - 1 - i) for i in range(n)]
    side = 1 - 2 * (lax.axis_index(axis) % 2)
    found, offsets = [], [0]
    one, two = shard, shard
    for step in range(1, n // 2):
        before = one
        one = lax.ppermute(two, axis, even)
        two = lax.ppermute(before, axis, odd)
        found += [one, two]
        offsets += [side * step, -side * step]
    first = lax.ppermute(two[:cut], axis, even)
    second = lax.ppermute(one[cut:], axis, odd)
    offsets.append(n // 2)
    owners = (lax.axis_index(axis) + jnp.stack([jnp.int32(k) for k in offsets])) % n
    return found, first, second, owners


def copy_for_each(shard, axis):
    n = lax.psum(1, axis)
    copies = jnp.broadcast_to(shard, (n, *shard.shape))
    return lax.all_to_all(copies, axis, split_axis=0, concat_axis=0, tiled=True)


def dot(a, b):
    return jnp.dot(a, b, preferred_element_type=jnp.float32)


def kernel_call(body, out_shape, flops, scratch=(), mib=16):
    vmem = pl.BlockSpec(memory_space=pltpu.VMEM)
    smem = pl.BlockSpec(memory_space=pltpu.SMEM)

    def call(scalars, *arrays):
        return pl.pallas_call(
            body,
            out_shape=out_shape,
            in_specs=[smem] * (scalars is not None) + [vmem] * len(arrays),
            out_specs=jax.tree.map(lambda _: vmem, out_shape),
            scratch_shapes=list(scratch),
            cost_estimate=pl.CostEstimate(flops=flops, bytes_accessed=1 << 20, transcendentals=0),
            compiler_params=pltpu.CompilerParams(vmem_limit_bytes=mib << 20),
        )(*(() if scalars is None else (scalars,)), *arrays)

    return call


def pack_kernel(places, *refs):
    sources, out_ref, sems = refs[:-2], refs[-2], refs[-1]
    copies = []
    for k, (source, left, at) in enumerate(places):
        ref = sources[source]
        copies.append(
            pltpu.make_async_copy(
                ref.at[:, pl.ds(left, out_ref.shape[1])],
                out_ref.at[pl.ds(at, ref.shape[0]), :],
                sems.at[k],
            )
        )
    for copy in copies:
        copy.start()
    for copy in copies:
        copy.wait()


def packed_rows(sources, width):
    places, at = [], 0
    for k, source in enumerate(sources):
        for left in range(0, source.shape[1], width):
            places.append((k, left, at))
            at += source.shape[0]
    return pl.pallas_call(
        functools.partial(pack_kernel, places),
        out_shape=jax.ShapeDtypeStruct((at, width), sources[0].dtype),
        in_specs=[pl.BlockSpec(memory_space=pltpu.HBM)] * len(sources),
        out_specs=pl.BlockSpec(memory_space=pltpu.VMEM),
        scratch_shapes=[pltpu.SemaphoreType.DMA((len(places),))],
    )(*sources)


def project_kernel(weight_ref, hidden_ref, out_ref):
    joined = jnp.concatenate([weight_ref[k] for k in range(weight_ref.shape[0])], axis=1)
    out_ref[...] = lax.dot_general(
        joined, hidden_ref[...], (((1,), (1,)), ((), ())), preferred_element_type=jnp.float32
    ).astype(out_ref.dtype)


def spread(block, owner, count):
    tall = jnp.concatenate([block] * count, axis=0)
    row = lax.broadcasted_iota(jnp.int32, tall.shape, 0)
    return tall, row // block.shape[0] == owner


def part_kernel(h, owner_ref, turned_ref, hidden_ref, *refs):
    shard_refs = refs[: h.count - 1]
    proj_ref, head_ref, one_ref, two_ref, three_ref, wide_ref = refs[h.count - 1 :]
    proj_ref[...] = turned_ref[...].T
    n, half = h.count, h.half
    last = owner_ref[n - 1]
    blank = jnp.zeros((h.one, half), wide_ref.dtype)
    small = jnp.zeros((h.two, half), wide_ref.dtype)
    for side in range(2):
        wide_ref[side, pl.ds(pl.multiple_of(last * h.one, h.one), h.one), :] = blank
        two_ref[side, pl.ds(pl.multiple_of(last * h.two, h.two), h.two), :] = small
    threes = [jnp.zeros((h.three * n, half), jnp.float32)] * 2
    head = None
    for k, ref in enumerate(shard_refs):
        owner = owner_ref[k]
        for side in range(2):
            wide_ref[side, pl.ds(pl.multiple_of(owner * h.one, h.one), h.one), :] = ref[
                side * h.one : (side + 1) * h.one, :
            ]
            at = 2 * h.one + side * h.two
            two_ref[side, pl.ds(pl.multiple_of(owner * h.two, h.two), h.two), :] = ref[
                at : at + h.two, :
            ]
        both = ref[h.three_at : h.head_at, :].astype(jnp.float32)
        for side in range(2):
            tall, there = spread(both[side * h.three : (side + 1) * h.three], owner, n)
            threes[side] = jnp.where(there, tall, threes[side])
        features = hidden_ref[:, pl.ds(pl.multiple_of(owner * h.head, h.head), h.head)]
        term = dot(features, ref[h.head_at :, :])
        head = term if head is None else head + term
    head_ref[...] = head
    for side in range(2):
        three_ref[side] = threes[side].astype(three_ref.dtype)
        one_ref[:, side * half : (side + 1) * half] = dot(
            proj_ref[:, : h.one * n], wide_ref[side]
        )


def last_kernel(
    h,
    owner_ref,
    first_ref,
    second_ref,
    hidden_ref,
    proj_ref,
    head_ref,
    one_ref,
    two_ref,
    three_ref,
    ids_ref,
    out_ref,
    wide_ref,
):
    n, half = h.count, h.half
    owner = owner_ref[n - 1]
    rows = hidden_ref.shape[0]
    rest = h.cut - h.head_at
    at = pl.multiple_of(owner * h.head, h.head)
    head = head_ref[...] + dot(hidden_ref[:, pl.ds(at, rest)], first_ref[h.head_at :, :])
    at = pl.multiple_of(owner * h.head + rest, 128)
    head = head + dot(hidden_ref[:, pl.ds(at, h.head - rest)], second_ref[...])
    one_features = proj_ref[:, pl.ds(pl.multiple_of(owner * h.one, h.one), h.one)]
    two_features = proj_ref[:, h.one * n : (h.one + h.two) * n]
    three_features = proj_ref[:, (h.one + h.two) * n : (h.one + h.two + h.three) * n]
    wide_ref[...] = two_ref[...]
    both = first_ref[h.three_at : h.head_at, :].astype(jnp.float32)
    ones, twos, threes = [], [], []
    for side in range(2):
        ones.append(
            one_ref[:, side * half : (side + 1) * half]
            + dot(one_features, first_ref[side * h.one : (side + 1) * h.one, :])
        )
        at = 2 * h.one + side * h.two
        wide_ref[side, pl.ds(pl.multiple_of(owner * h.two, h.two), h.two), :] = first_ref[
            at : at + h.two, :
        ]
        twos.append(dot(two_features, wide_ref[side]))
        tall, there = spread(both[side * h.three : (side + 1) * h.three], owner, n)
        block = jnp.where(there, tall, three_ref[side].astype(jnp.float32))
        threes.append(dot(three_features, block.astype(three_ref.dtype)))
    columns = []
    pick = jnp.zeros((rows, 1), jnp.float32)
    tops, sums, weighted = [], [], []
    for k, sides in enumerate(([head], ones, twos, threes)):
        top = functools.reduce(
            jnp.maximum, [jnp.max(logits, axis=1, keepdims=True) for logits in sides]
        )
        total = jnp.zeros((rows, 1), jnp.float32)
        mass = jnp.zeros((rows, 1), jnp.float32)
        for side, logits in enumerate(sides):
            expo = jnp.exp(logits - top)
            total = total + jnp.sum(expo, axis=1, keepdims=True)
            if k:
                mass = mass + jnp.sum(expo * logits, axis=1, keepdims=True)
            word = lax.broadcasted_iota(jnp.int32, logits.shape, 1) + side * half
            hit = word == ids_ref[:, k : k + 1]
            pick = pick + jnp.sum(jnp.where(hit, logits, 0.0), axis=1, keepdims=True)
        tops.append(top)
        sums.append(total)
        if k:
            weighted.append(mass)
    columns = [*tops, *sums, *weighted, pick]
    lane = lax.broadcasted_iota(jnp.int32, (rows, 128), 1)
    table = jnp.zeros((rows, 128), jnp.float32)
    for k, column in enumerate(columns):
        table = jnp.where(lane == k, column, table)
    write_copies(table.T, out_ref)


def write_copies(table, out_ref):
    width = out_ref.shape[2] // 12
    for k in range(12):
        out_ref[:, 0, k * width : (k + 1) * width] = jnp.broadcast_to(
            table[k : k + 1], (out_ref.shape[0], width)
        )


def combined(ref):
    width = ref.shape[2] // 12
    rows = [ref[:, 0, k * width : (k + 1) * width] for k in range(12)]

    def down(combine, array):
        return combine(array, axis=0, keepdims=True)

    tops = [down(jnp.max, row) for row in rows[0:4]]
    scales = [jnp.exp(row - top) for row, top in zip(rows[0:4], tops)]
    sums = [down(jnp.sum, row * scale) for row, scale in zip(rows[4:8], scales)]
    masses = [down(jnp.sum, row * scale) for row, scale in zip(rows[8:11], scales[1:])]
    return [*tops, *sums, *masses, down(jnp.sum, rows[11])]


def merge_kernel(stats_ref, out_ref):
    write_copies(jnp.concatenate(combined(stats_ref), axis=0), out_ref)


def finish_kernel(stats_ref, scores_ref, flags_ref, targets_ref, prob_ref, entropy_ref):
    rows = combined(stats_ref)
    scores, flags, targets = scores_ref[...], flags_ref[...], targets_ref[...]
    top = jnp.maximum(rows[0], jnp.max(scores, axis=0, keepdims=True))
    total = rows[4] * jnp.exp(rows[0] - top) + jnp.sum(
        jnp.exp(scores - top), axis=0, keepdims=True
    )
    head_lse = top + jnp.log(total)
    picked = rows[11]
    for k in range(3):
        lse = rows[1 + k] + jnp.log(rows[5 + k])
        mean = rows[8 + k] / rows[5 + k]
        entropy_ref[k : k + 1, :] = flags[k : k + 1].astype(jnp.float32) * (lse - mean)
        low = V_HEAD + k * TAIL
        inside = jnp.logical_and(targets >= low, targets < low + TAIL)
        picked = picked + jnp.where(inside, scores[k : k + 1] - lse, 0.0)
    prob_ref[...] = picked - head_lse


class Heights:
    def __init__(self, count, one, two, three, head, half):
        self.count, self.one, self.two, self.three = count, one, two, three
        self.head, self.half = head, half
        self.three_at = 2 * (one + two)
        self.head_at = 2 * (one + two + three)
        self.cut = self.head_at + 128


def one_device(
    hidden,
    head_weight,
    cluster_weight,
    proj_one,
    proj_two,
    proj_three,
    tail_one,
    tail_two,
    tail_three,
    targets,
    flags,
):
    rows = hidden.shape[0]
    head_cols = head_weight.shape[1]
    tail_cols = tail_one.shape[1]
    half = tail_cols // 2
    n_chips = lax.psum(1, CHIPS)
    n_grp = lax.axis_size("grp")
    core = lax.axis_index(CORE)
    vocab_index = lax.axis_index(VOCAB)

    tails = (tail_one, tail_two, tail_three)
    h = Heights(n_grp, *(t.shape[0] for t in tails), head_weight.shape[0], half)
    packed = packed_rows((*tails, head_weight), half)
    found, first, second, owners = ring(packed, "grp", h.cut)

    widths = (proj_one.shape[1], proj_two.shape[1], proj_three.shape[1])
    total = sum(widths)
    share = -(-total // (2 * n_chips) // 8) * 8
    joined = lax.all_gather(
        jnp.concatenate((proj_one, proj_two, proj_three), axis=1), CORE, axis=0, tiled=True
    )
    turned = jnp.pad(joined.T, ((0, 2 * n_chips * share - total), (0, 0)))
    turned = turned.reshape(2, n_chips, share, joined.shape[0])
    pieces = lax.dynamic_index_in_dim(turned, core, 0, keepdims=False)
    pieces = lax.all_to_all(pieces, CHIPS, split_axis=0, concat_axis=0, tiled=True)
    mine = kernel_call(
        project_kernel,
        jax.ShapeDtypeStruct((share, rows), jnp.bfloat16),
        2 * share * hidden.size,
    )(None, pieces, hidden)
    turned = copy_for_each(mine, CHIPS)
    turned = lax.all_gather(turned, CORE)
    turned = turned.reshape(2 * n_chips * share, rows)

    wide = jnp.bfloat16
    part_call = kernel_call(
        functools.partial(part_kernel, h),
        (
            jax.ShapeDtypeStruct((rows, turned.shape[0]), wide),
            jax.ShapeDtypeStruct((rows, head_cols), jnp.float32),
            jax.ShapeDtypeStruct((rows, tail_cols), jnp.float32),
            jax.ShapeDtypeStruct((2, h.two * n_grp, half), wide),
            jax.ShapeDtypeStruct((2, h.three * n_grp, half), wide),
        ),
        2 * rows * packed.size * n_grp,
        [pltpu.VMEM((2, h.one * n_grp, half), wide)],
    )
    part = part_call(owners, turned, hidden, packed, *found)

    cluster_logits = dot(hidden, cluster_weight)
    relative = targets - V_HEAD
    cluster = relative // TAIL
    word = relative - cluster * TAIL
    ids = jnp.stack(
        [targets - vocab_index * head_cols]
        + [jnp.where(cluster == k, word - vocab_index * tail_cols, -1) for k in range(3)],
        axis=1,
    )
    near = VOCAB[1:]
    n_near = lax.psum(1, near)
    n_far = lax.axis_size(VOCAB[0])
    stats = kernel_call(
        functools.partial(last_kernel, h),
        jax.ShapeDtypeStruct((n_near, 1, 12 * rows), jnp.float32),
        2 * rows * packed.size,
        [pltpu.VMEM((2, h.two * n_grp, half), wide)],
    )(owners, first, second, hidden, *part, ids)
    stats = lax.all_to_all(stats, near, split_axis=0, concat_axis=0, tiled=True)
    stats = kernel_call(
        merge_kernel, jax.ShapeDtypeStruct((n_far, 1, 12 * rows), jnp.float32), 1 << 20, mib=4
    )(None, stats)
    stats = lax.all_to_all(stats, VOCAB[0], split_axis=0, concat_axis=0, tiled=True)
    target_logprob, entropy = kernel_call(
        finish_kernel,
        (
            jax.ShapeDtypeStruct((1, rows), jnp.float32),
            jax.ShapeDtypeStruct((3, rows), jnp.float32),
        ),
        1 << 20,
        mib=4,
    )(None, stats, cluster_logits.T, flags.T, targets[None])
    return (target_logprob[0], entropy.T)


def solution(mesh):
    finer = Mesh(
        mesh.devices.reshape(8, 4, 2, mesh.shape["grp"]), ("vocab_0", "vocab_1", "vocab_2", "grp")
    )
    in_specs = (
        P("grp", None),
        P("grp", VOCAB),
        P(),
        P(VOCAB, None),
        P(VOCAB, None),
        P(VOCAB, None),
        P("grp", VOCAB),
        P("grp", VOCAB),
        P("grp", VOCAB),
        P("grp"),
        P("grp", None),
    )
    out_specs = (P("grp"), P("grp", None))
    return jax.shard_map(
        one_device, mesh=finer, in_specs=in_specs, out_specs=out_specs, check_vma=False
    )
```

```python
import functools

import jax
import jax.numpy as jnp
from jax import lax
from jax.experimental import pallas as pl
from jax.experimental.pallas import tpu as pltpu
from jax.sharding import Mesh
from jax.sharding import PartitionSpec as P


V_HEAD = 32768
TAIL = 65536
VOCAB = ("vocab_0", "vocab_1", "vocab_2")
CHIPS, CORE = VOCAB[:2], VOCAB[2]


def ring(shard, other, axis):
    n = lax.axis_size(axis)
    even = [(i, i ^ 1) for i in range(n)]
    odd = [(i, ((i + 1) ^ 1) - 1 if 0 < i < n - 1 else n - 1 - i) for i in range(n)]
    side = 1 - 2 * (lax.axis_index(axis) % 2)
    streams = {"a": (shard, shard), "b": (other, other)}
    found, offsets = {"a": [], "b": []}, [0]
    for step in range(1, n // 2):
        for name, (one, two) in streams.items():
            came = lax.ppermute(two, axis, even)
            two = lax.ppermute(one, axis, odd)
            streams[name] = (came, two)
            found[name] += [came, two]
        offsets += [side * step, -side * step]
    first = lax.ppermute(streams["a"][1], axis, even)
    second = lax.ppermute(streams["b"][0], axis, odd)
    offsets.append(n // 2)
    owners = (lax.axis_index(axis) + jnp.stack([jnp.int32(k) for k in offsets])) % n
    return found["a"], found["b"], first, second, owners


def copy_for_each(shard, axis):
    n = lax.psum(1, axis)
    copies = jnp.broadcast_to(shard, (n, *shard.shape))
    return lax.all_to_all(copies, axis, split_axis=0, concat_axis=0, tiled=True)


def dot(a, b):
    return jnp.dot(a, b, preferred_element_type=jnp.float32)


def kernel_call(body, out_shape, flops, scratch=(), mib=16):
    vmem = pl.BlockSpec(memory_space=pltpu.VMEM)
    smem = pl.BlockSpec(memory_space=pltpu.SMEM)

    def call(scalars, *arrays):
        return pl.pallas_call(
            body,
            out_shape=out_shape,
            in_specs=[smem] * (scalars is not None) + [vmem] * len(arrays),
            out_specs=jax.tree.map(lambda _: vmem, out_shape),
            scratch_shapes=list(scratch),
            cost_estimate=pl.CostEstimate(flops=flops, bytes_accessed=1 << 20, transcendentals=0),
            compiler_params=pltpu.CompilerParams(vmem_limit_bytes=mib << 20),
        )(*(() if scalars is None else (scalars,)), *arrays)

    return call


def pack_kernel(places, *refs):
    sources, outs, sems = refs[:-3], refs[-3:-1], refs[-1]
    copies = []
    for k, (source, top, height, left, out, at) in enumerate(places):
        copies.append(
            pltpu.make_async_copy(
                sources[source].at[pl.ds(top, height), pl.ds(left, outs[out].shape[1])],
                outs[out].at[pl.ds(at, height), :],
                sems.at[k],
            )
        )
    for copy in copies:
        copy.start()
    for copy in copies:
        copy.wait()


def packed_rows(tails, head, width, rest):
    places, at = [], 0
    for k, tail in enumerate(tails):
        for left in range(0, tail.shape[1], width):
            places.append((k, 0, tail.shape[0], left, 0, at))
            at += tail.shape[0]
    places.append((len(tails), 0, rest, 0, 0, at))
    places.append((len(tails), rest, head.shape[0] - rest, 0, 1, 0))
    return pl.pallas_call(
        functools.partial(pack_kernel, places),
        out_shape=(
            jax.ShapeDtypeStruct((at + rest, width), head.dtype),
            jax.ShapeDtypeStruct((head.shape[0] - rest, width), head.dtype),
        ),
        in_specs=[pl.BlockSpec(memory_space=pltpu.HBM)] * (len(tails) + 1),
        out_specs=(pl.BlockSpec(memory_space=pltpu.VMEM),) * 2,
        scratch_shapes=[pltpu.SemaphoreType.DMA((len(places),))],
    )(*tails, head)


def project_kernel(weight_ref, hidden_ref, out_ref):
    joined = jnp.concatenate([weight_ref[k] for k in range(weight_ref.shape[0])], axis=1)
    out_ref[...] = lax.dot_general(
        joined, hidden_ref[...], (((1,), (1,)), ((), ())), preferred_element_type=jnp.float32
    ).astype(out_ref.dtype)


def spread(block, owner, count):
    tall = jnp.concatenate([block] * count, axis=0)
    row = lax.broadcasted_iota(jnp.int32, tall.shape, 0)
    return tall, row // block.shape[0] == owner


def part_kernel(h, owner_ref, hidden_ref, *refs):
    *refs, head_ref = refs
    count = h.count - 1
    head = None
    for k in range(count):
        for low, block in ((0, refs[k][h.head_at :, :]), (h.rest, refs[count + k][...])):
            at = pl.multiple_of(owner_ref[k] * h.head + low, 128)
            term = dot(hidden_ref[:, pl.ds(at, block.shape[0])], block)
            head = term if head is None else head + term
    head_ref[...] = head


def lift_kernel(h, owner_ref, turned_ref, *refs):
    shard_refs = refs[: h.count - 1]
    proj_ref, one_ref, two_ref, three_ref, wide_ref = refs[h.count - 1 :]
    proj_ref[...] = turned_ref[...].T
    n, half = h.count, h.half
    last = owner_ref[n - 1]
    blank = jnp.zeros((h.one, half), wide_ref.dtype)
    small = jnp.zeros((h.two, half), wide_ref.dtype)
    for side in range(2):
        wide_ref[side, pl.ds(pl.multiple_of(last * h.one, h.one), h.one), :] = blank
        two_ref[side, pl.ds(pl.multiple_of(last * h.two, h.two), h.two), :] = small
    threes = [jnp.zeros((h.three * n, half), jnp.float32)] * 2
    for k, ref in enumerate(shard_refs):
        owner = owner_ref[k]
        for side in range(2):
            wide_ref[side, pl.ds(pl.multiple_of(owner * h.one, h.one), h.one), :] = ref[
                side * h.one : (side + 1) * h.one, :
            ]
            at = 2 * h.one + side * h.two
            two_ref[side, pl.ds(pl.multiple_of(owner * h.two, h.two), h.two), :] = ref[
                at : at + h.two, :
            ]
        both = ref[h.three_at : h.head_at, :].astype(jnp.float32)
        for side in range(2):
            tall, there = spread(both[side * h.three : (side + 1) * h.three], owner, n)
            threes[side] = jnp.where(there, tall, threes[side])
    for side in range(2):
        three_ref[side] = threes[side].astype(three_ref.dtype)
        one_ref[:, side * half : (side + 1) * half] = dot(
            proj_ref[:, : h.one * n], wide_ref[side]
        )


def columns_of(sides, ids, with_mass):
    top = functools.reduce(
        jnp.maximum, [jnp.max(logits, axis=1, keepdims=True) for logits in sides]
    )
    total = mass = pick = jnp.zeros_like(top)
    for side, logits in enumerate(sides):
        expo = jnp.exp(logits - top)
        total = total + jnp.sum(expo, axis=1, keepdims=True)
        if with_mass:
            mass = mass + jnp.sum(expo * logits, axis=1, keepdims=True)
        word = lax.broadcasted_iota(jnp.int32, logits.shape, 1) + side * logits.shape[1]
        pick = pick + jnp.sum(jnp.where(word == ids, logits, 0.0), axis=1, keepdims=True)
    return top, total, mass, pick


def tails_kernel(
    h,
    owner_ref,
    first_ref,
    hidden_ref,
    proj_ref,
    head_ref,
    one_ref,
    two_ref,
    three_ref,
    ids_ref,
    table_ref,
    more_ref,
    wide_ref,
):
    n, half = h.count, h.half
    owner = owner_ref[n - 1]
    rows = hidden_ref.shape[0]
    at = pl.multiple_of(owner * h.head, h.head)
    more_ref[...] = head_ref[...] + dot(
        hidden_ref[:, pl.ds(at, h.rest)], first_ref[h.head_at :, :]
    )
    one_features = proj_ref[:, pl.ds(pl.multiple_of(owner * h.one, h.one), h.one)]
    two_features = proj_ref[:, h.one * n : (h.one + h.two) * n]
    three_features = proj_ref[:, (h.one + h.two) * n : (h.one + h.two + h.three) * n]
    wide_ref[...] = two_ref[...]
    both = first_ref[h.three_at : h.head_at, :].astype(jnp.float32)
    ones, twos, threes = [], [], []
    for side in range(2):
        ones.append(
            one_ref[:, side * half : (side + 1) * half]
            + dot(one_features, first_ref[side * h.one : (side + 1) * h.one, :])
        )
        at = 2 * h.one + side * h.two
        wide_ref[side, pl.ds(pl.multiple_of(owner * h.two, h.two), h.two), :] = first_ref[
            at : at + h.two, :
        ]
        twos.append(dot(two_features, wide_ref[side]))
        tall, there = spread(both[side * h.three : (side + 1) * h.three], owner, n)
        block = jnp.where(there, tall, three_ref[side].astype(jnp.float32))
        threes.append(dot(three_features, block.astype(three_ref.dtype)))
    lane = lax.broadcasted_iota(jnp.int32, (rows, 128), 1)
    table = jnp.zeros((rows, 128), jnp.float32)
    picked = jnp.zeros((rows, 1), jnp.float32)
    for k, sides in enumerate((ones, twos, threes)):
        top, total, mass, pick = columns_of(sides, ids_ref[:, 1 + k : 2 + k], True)
        for place, column in ((1 + k, top), (5 + k, total), (8 + k, mass)):
            table = jnp.where(lane == place, column, table)
        picked = picked + pick
    table_ref[...] = jnp.where(lane == 11, picked, table)


def last_kernel(h, owner_ref, second_ref, hidden_ref, head_ref, table_ref, ids_ref, out_ref):
    at = pl.multiple_of(owner_ref[h.count - 1] * h.head + h.rest, 128)
    head = head_ref[...] + dot(
        hidden_ref[:, pl.ds(at, h.head - h.rest)], second_ref[...]
    )
    top, total, _, pick = columns_of([head], ids_ref[:, 0:1], False)
    table = table_ref[...]
    lane = lax.broadcasted_iota(jnp.int32, table.shape, 1)
    table = jnp.where(lane == 0, top, jnp.where(lane == 4, total, table))
    write_copies((table + jnp.where(lane == 11, pick, 0.0)).T, out_ref)


def write_copies(table, out_ref):
    width = out_ref.shape[2] // 12
    for k in range(12):
        out_ref[:, 0, k * width : (k + 1) * width] = jnp.broadcast_to(
            table[k : k + 1], (out_ref.shape[0], width)
        )


def combined(ref):
    width = ref.shape[2] // 12
    rows = [ref[:, 0, k * width : (k + 1) * width] for k in range(12)]

    def down(combine, array):
        return combine(array, axis=0, keepdims=True)

    tops = [down(jnp.max, row) for row in rows[0:4]]
    scales = [jnp.exp(row - top) for row, top in zip(rows[0:4], tops)]
    sums = [down(jnp.sum, row * scale) for row, scale in zip(rows[4:8], scales)]
    masses = [down(jnp.sum, row * scale) for row, scale in zip(rows[8:11], scales[1:])]
    return [*tops, *sums, *masses, down(jnp.sum, rows[11])]


def merge_kernel(stats_ref, out_ref):
    write_copies(jnp.concatenate(combined(stats_ref), axis=0), out_ref)


def finish_kernel(stats_ref, scores_ref, flags_ref, targets_ref, prob_ref, entropy_ref):
    rows = combined(stats_ref)
    scores, flags, targets = scores_ref[...], flags_ref[...], targets_ref[...]
    top = jnp.maximum(rows[0], jnp.max(scores, axis=0, keepdims=True))
    total = rows[4] * jnp.exp(rows[0] - top) + jnp.sum(
        jnp.exp(scores - top), axis=0, keepdims=True
    )
    head_lse = top + jnp.log(total)
    picked = rows[11]
    for k in range(3):
        lse = rows[1 + k] + jnp.log(rows[5 + k])
        mean = rows[8 + k] / rows[5 + k]
        entropy_ref[k : k + 1, :] = flags[k : k + 1].astype(jnp.float32) * (lse - mean)
        low = V_HEAD + k * TAIL
        inside = jnp.logical_and(targets >= low, targets < low + TAIL)
        picked = picked + jnp.where(inside, scores[k : k + 1] - lse, 0.0)
    prob_ref[...] = picked - head_lse


class Heights:
    def __init__(self, count, one, two, three, head, half):
        self.count, self.one, self.two, self.three = count, one, two, three
        self.head, self.half = head, half
        self.three_at = 2 * (one + two)
        self.head_at = 2 * (one + two + three)
        self.rest = 128


def one_device(
    hidden,
    head_weight,
    cluster_weight,
    proj_one,
    proj_two,
    proj_three,
    tail_one,
    tail_two,
    tail_three,
    targets,
    flags,
):
    rows = hidden.shape[0]
    head_cols = head_weight.shape[1]
    tail_cols = tail_one.shape[1]
    half = tail_cols // 2
    n_chips = lax.psum(1, CHIPS)
    n_grp = lax.axis_size("grp")
    core = lax.axis_index(CORE)
    vocab_index = lax.axis_index(VOCAB)

    tails = (tail_one, tail_two, tail_three)
    h = Heights(n_grp, *(t.shape[0] for t in tails), head_weight.shape[0], half)
    shard, other = packed_rows(tails, head_weight, half, h.rest)
    found, others, first, second, owners = ring(shard, other, "grp")

    widths = (proj_one.shape[1], proj_two.shape[1], proj_three.shape[1])
    total = sum(widths)
    share = -(-total // (2 * n_chips) // 8) * 8
    joined = lax.all_gather(
        jnp.concatenate((proj_one, proj_two, proj_three), axis=1), CORE, axis=0, tiled=True
    )
    turned = jnp.pad(joined.T, ((0, 2 * n_chips * share - total), (0, 0)))
    turned = turned.reshape(2, n_chips, share, joined.shape[0])
    pieces = lax.dynamic_index_in_dim(turned, core, 0, keepdims=False)
    pieces = lax.all_to_all(pieces, CHIPS, split_axis=0, concat_axis=0, tiled=True)
    mine = kernel_call(
        project_kernel,
        jax.ShapeDtypeStruct((share, rows), jnp.bfloat16),
        2 * share * hidden.size,
    )(None, pieces, hidden)
    turned = copy_for_each(mine, CHIPS)
    turned = lax.all_gather(turned, CORE)
    turned = turned.reshape(2 * n_chips * share, rows)

    wide = jnp.bfloat16
    part_call = kernel_call(
        functools.partial(part_kernel, h),
        jax.ShapeDtypeStruct((rows, head_cols), jnp.float32),
        2 * rows * head_weight.size * n_grp,
    )
    head_part = part_call(owners, hidden, shard, *found, other, *others)
    lift_call = kernel_call(
        functools.partial(lift_kernel, h),
        (
            jax.ShapeDtypeStruct((rows, turned.shape[0]), wide),
            jax.ShapeDtypeStruct((rows, tail_cols), jnp.float32),
            jax.ShapeDtypeStruct((2, h.two * n_grp, half), wide),
            jax.ShapeDtypeStruct((2, h.three * n_grp, half), wide),
        ),
        2 * rows * tail_one.size * n_grp,
        [pltpu.VMEM((2, h.one * n_grp, half), wide)],
    )
    proj, one_part, *small_rows = lift_call(owners, turned, shard, *found)

    cluster_logits = dot(hidden, cluster_weight)
    relative = targets - V_HEAD
    cluster = relative // TAIL
    word = relative - cluster * TAIL
    ids = jnp.stack(
        [targets - vocab_index * head_cols]
        + [jnp.where(cluster == k, word - vocab_index * tail_cols, -1) for k in range(3)],
        axis=1,
    )
    near = VOCAB[1:]
    n_near = lax.psum(1, near)
    n_far = lax.axis_size(VOCAB[0])
    tails_call = kernel_call(
        functools.partial(tails_kernel, h),
        (
            jax.ShapeDtypeStruct((rows, 128), jnp.float32),
            jax.ShapeDtypeStruct((rows, head_cols), jnp.float32),
        ),
        2 * rows * shard.size,
        [pltpu.VMEM((2, h.two * n_grp, half), wide)],
    )
    table, head_part = tails_call(
        owners, first, hidden, proj, head_part, one_part, *small_rows, ids
    )
    stats = kernel_call(
        functools.partial(last_kernel, h),
        jax.ShapeDtypeStruct((n_near, 1, 12 * rows), jnp.float32),
        2 * rows * other.size,
        mib=8,
    )(owners, second, hidden, head_part, table, ids)
    stats = lax.all_to_all(stats, near, split_axis=0, concat_axis=0, tiled=True)
    stats = kernel_call(
        merge_kernel, jax.ShapeDtypeStruct((n_far, 1, 12 * rows), jnp.float32), 1 << 20, mib=4
    )(None, stats)
    stats = lax.all_to_all(stats, VOCAB[0], split_axis=0, concat_axis=0, tiled=True)
    target_logprob, entropy = kernel_call(
        finish_kernel,
        (
            jax.ShapeDtypeStruct((1, rows), jnp.float32),
            jax.ShapeDtypeStruct((3, rows), jnp.float32),
        ),
        1 << 20,
        mib=4,
    )(None, stats, cluster_logits.T, flags.T, targets[None])
    return (target_logprob[0], entropy.T)


def solution(mesh):
    finer = Mesh(
        mesh.devices.reshape(8, 4, 2, mesh.shape["grp"]), ("vocab_0", "vocab_1", "vocab_2", "grp")
    )
    in_specs = (
        P("grp", None),
        P("grp", VOCAB),
        P(),
        P(VOCAB, None),
        P(VOCAB, None),
        P(VOCAB, None),
        P("grp", VOCAB),
        P("grp", VOCAB),
        P("grp", VOCAB),
        P("grp"),
        P("grp", None),
    )
    out_specs = (P("grp"), P("grp", None))
    return jax.shard_map(
        one_device, mesh=finer, in_specs=in_specs, out_specs=out_specs, check_vma=False
    )
```

```python
import functools

import jax
import jax.numpy as jnp
from jax import lax
from jax.experimental import pallas as pl
from jax.experimental.pallas import tpu as pltpu
from jax.sharding import Mesh
from jax.sharding import PartitionSpec as P


V_HEAD = 32768
TAIL = 65536
VOCAB = ("vocab_0", "vocab_1", "vocab_2")
CHIPS, CORE = VOCAB[:2], VOCAB[2]


def ring(shard, other, axis):
    n = lax.axis_size(axis)
    even = [(i, i ^ 1) for i in range(n)]
    odd = [(i, ((i + 1) ^ 1) - 1 if 0 < i < n - 1 else n - 1 - i) for i in range(n)]
    side = 1 - 2 * (lax.axis_index(axis) % 2)
    streams = {"a": (shard, shard), "b": (other, other)}
    found, offsets = {"a": [], "b": []}, [0]
    for step in range(1, n // 2):
        for name, (one, two) in streams.items():
            came = lax.ppermute(two, axis, even)
            two = lax.ppermute(one, axis, odd)
            streams[name] = (came, two)
            found[name] += [came, two]
        offsets += [side * step, -side * step]
    first = lax.ppermute(streams["a"][1], axis, even)
    second = lax.ppermute(streams["b"][0], axis, odd)
    offsets.append(n // 2)
    owners = (lax.axis_index(axis) + jnp.stack([jnp.int32(k) for k in offsets])) % n
    return found["a"], found["b"], first, second, owners


def copy_for_each(shard, axis):
    n = lax.psum(1, axis)
    copies = jnp.broadcast_to(shard, (n, *shard.shape))
    return lax.all_to_all(copies, axis, split_axis=0, concat_axis=0, tiled=True)


def dot(a, b):
    return jnp.dot(a, b, preferred_element_type=jnp.float32)


def kernel_call(body, out_shape, flops, scratch=(), mib=16):
    vmem = pl.BlockSpec(memory_space=pltpu.VMEM)
    smem = pl.BlockSpec(memory_space=pltpu.SMEM)

    def call(scalars, *arrays):
        return pl.pallas_call(
            body,
            out_shape=out_shape,
            in_specs=[smem] * (scalars is not None) + [vmem] * len(arrays),
            out_specs=jax.tree.map(lambda _: vmem, out_shape),
            scratch_shapes=list(scratch),
            cost_estimate=pl.CostEstimate(flops=flops, bytes_accessed=1 << 20, transcendentals=0),
            compiler_params=pltpu.CompilerParams(vmem_limit_bytes=mib << 20),
        )(*(() if scalars is None else (scalars,)), *arrays)

    return call


def pack_kernel(places, *refs):
    sources, outs, sems = refs[:-3], refs[-3:-1], refs[-1]
    copies = []
    for k, (source, top, height, left, out, at) in enumerate(places):
        copies.append(
            pltpu.make_async_copy(
                sources[source].at[pl.ds(top, height), pl.ds(left, outs[out].shape[1])],
                outs[out].at[pl.ds(at, height), :],
                sems.at[k],
            )
        )
    for copy in copies:
        copy.start()
    for copy in copies:
        copy.wait()


def packed_rows(tails, head, width, rest):
    places, at = [], 0
    for k, tail in enumerate(tails):
        for left in range(0, tail.shape[1], width):
            places.append((k, 0, tail.shape[0], left, 0, at))
            at += tail.shape[0]
    places.append((len(tails), 0, rest, 0, 0, at))
    places.append((len(tails), rest, head.shape[0] - rest, 0, 1, 0))
    return pl.pallas_call(
        functools.partial(pack_kernel, places),
        out_shape=(
            jax.ShapeDtypeStruct((at + rest, width), head.dtype),
            jax.ShapeDtypeStruct((head.shape[0] - rest, width), head.dtype),
        ),
        in_specs=[pl.BlockSpec(memory_space=pltpu.HBM)] * (len(tails) + 1),
        out_specs=(pl.BlockSpec(memory_space=pltpu.VMEM),) * 2,
        scratch_shapes=[pltpu.SemaphoreType.DMA((len(places),))],
    )(*tails, head)


def project_kernel(weight_ref, hidden_ref, out_ref):
    joined = jnp.concatenate([weight_ref[k] for k in range(weight_ref.shape[0])], axis=1)
    out_ref[...] = lax.dot_general(
        joined, hidden_ref[...], (((1,), (1,)), ((), ())), preferred_element_type=jnp.float32
    ).astype(out_ref.dtype)


def spread(block, owner, count):
    tall = jnp.concatenate([block] * count, axis=0)
    row = lax.broadcasted_iota(jnp.int32, tall.shape, 0)
    return tall, row // block.shape[0] == owner


def part_kernel(h, owner_ref, turned_ref, hidden_ref, *refs):
    shard_refs = refs[: h.count - 1]
    other_refs = refs[h.count - 1 : 2 * h.count - 2]
    proj_ref, head_ref, one_ref, two_ref, three_ref, wide_ref = refs[2 * h.count - 2 :]
    proj_ref[...] = turned_ref[...].T
    n, half = h.count, h.half
    last = owner_ref[n - 1]
    blank = jnp.zeros((h.one, half), wide_ref.dtype)
    small = jnp.zeros((h.two, half), wide_ref.dtype)
    for side in range(2):
        wide_ref[side, pl.ds(pl.multiple_of(last * h.one, h.one), h.one), :] = blank
        two_ref[side, pl.ds(pl.multiple_of(last * h.two, h.two), h.two), :] = small
    threes = [jnp.zeros((h.three * n, half), jnp.float32)] * 2
    head = None
    for k, (ref, other) in enumerate(zip(shard_refs, other_refs)):
        owner = owner_ref[k]
        for side in range(2):
            wide_ref[side, pl.ds(pl.multiple_of(owner * h.one, h.one), h.one), :] = ref[
                side * h.one : (side + 1) * h.one, :
            ]
            at = 2 * h.one + side * h.two
            two_ref[side, pl.ds(pl.multiple_of(owner * h.two, h.two), h.two), :] = ref[
                at : at + h.two, :
            ]
        both = ref[h.three_at : h.head_at, :].astype(jnp.float32)
        for side in range(2):
            tall, there = spread(both[side * h.three : (side + 1) * h.three], owner, n)
            threes[side] = jnp.where(there, tall, threes[side])
        for low, block in ((0, ref[h.head_at :, :]), (h.rest, other[...])):
            at = pl.multiple_of(owner * h.head + low, 128)
            term = dot(hidden_ref[:, pl.ds(at, block.shape[0])], block)
            head = term if head is None else head + term
    head_ref[...] = head
    for side in range(2):
        three_ref[side] = threes[side].astype(three_ref.dtype)
        one_ref[:, side * half : (side + 1) * half] = dot(
            proj_ref[:, : h.one * n], wide_ref[side]
        )


def columns_of(sides, ids, with_mass):
    top = functools.reduce(
        jnp.maximum, [jnp.max(logits, axis=1, keepdims=True) for logits in sides]
    )
    total = mass = pick = jnp.zeros_like(top)
    for side, logits in enumerate(sides):
        expo = jnp.exp(logits - top)
        total = total + jnp.sum(expo, axis=1, keepdims=True)
        if with_mass:
            mass = mass + jnp.sum(expo * logits, axis=1, keepdims=True)
        word = lax.broadcasted_iota(jnp.int32, logits.shape, 1) + side * logits.shape[1]
        pick = pick + jnp.sum(jnp.where(word == ids, logits, 0.0), axis=1, keepdims=True)
    return top, total, mass, pick


def tails_kernel(
    h,
    owner_ref,
    first_ref,
    hidden_ref,
    proj_ref,
    head_ref,
    one_ref,
    two_ref,
    three_ref,
    ids_ref,
    table_ref,
    more_ref,
    wide_ref,
):
    n, half = h.count, h.half
    owner = owner_ref[n - 1]
    rows = hidden_ref.shape[0]
    at = pl.multiple_of(owner * h.head, h.head)
    more_ref[...] = head_ref[...] + dot(
        hidden_ref[:, pl.ds(at, h.rest)], first_ref[h.head_at :, :]
    )
    one_features = proj_ref[:, pl.ds(pl.multiple_of(owner * h.one, h.one), h.one)]
    two_features = proj_ref[:, h.one * n : (h.one + h.two) * n]
    three_features = proj_ref[:, (h.one + h.two) * n : (h.one + h.two + h.three) * n]
    wide_ref[...] = two_ref[...]
    both = first_ref[h.three_at : h.head_at, :].astype(jnp.float32)
    ones, twos, threes = [], [], []
    for side in range(2):
        ones.append(
            one_ref[:, side * half : (side + 1) * half]
            + dot(one_features, first_ref[side * h.one : (side + 1) * h.one, :])
        )
        at = 2 * h.one + side * h.two
        wide_ref[side, pl.ds(pl.multiple_of(owner * h.two, h.two), h.two), :] = first_ref[
            at : at + h.two, :
        ]
        twos.append(dot(two_features, wide_ref[side]))
        tall, there = spread(both[side * h.three : (side + 1) * h.three], owner, n)
        block = jnp.where(there, tall, three_ref[side].astype(jnp.float32))
        threes.append(dot(three_features, block.astype(three_ref.dtype)))
    lane = lax.broadcasted_iota(jnp.int32, (rows, 128), 1)
    table = jnp.zeros((rows, 128), jnp.float32)
    picked = jnp.zeros((rows, 1), jnp.float32)
    for k, sides in enumerate((ones, twos, threes)):
        top, total, mass, pick = columns_of(sides, ids_ref[:, 1 + k : 2 + k], True)
        for place, column in ((1 + k, top), (5 + k, total), (8 + k, mass)):
            table = jnp.where(lane == place, column, table)
        picked = picked + pick
    table_ref[...] = jnp.where(lane == 11, picked, table)


def last_kernel(h, owner_ref, second_ref, hidden_ref, head_ref, table_ref, ids_ref, out_ref):
    at = pl.multiple_of(owner_ref[h.count - 1] * h.head + h.rest, 128)
    head = head_ref[...] + dot(
        hidden_ref[:, pl.ds(at, h.head - h.rest)], second_ref[...]
    )
    top, total, _, pick = columns_of([head], ids_ref[:, 0:1], False)
    table = table_ref[...]
    lane = lax.broadcasted_iota(jnp.int32, table.shape, 1)
    table = jnp.where(lane == 0, top, jnp.where(lane == 4, total, table))
    write_copies((table + jnp.where(lane == 11, pick, 0.0)).T, out_ref)


def write_copies(table, out_ref):
    width = out_ref.shape[2] // 12
    for k in range(12):
        out_ref[:, 0, k * width : (k + 1) * width] = jnp.broadcast_to(
            table[k : k + 1], (out_ref.shape[0], width)
        )


def combined(ref):
    width = ref.shape[2] // 12
    rows = [ref[:, 0, k * width : (k + 1) * width] for k in range(12)]

    def down(combine, array):
        return combine(array, axis=0, keepdims=True)

    tops = [down(jnp.max, row) for row in rows[0:4]]
    scales = [jnp.exp(row - top) for row, top in zip(rows[0:4], tops)]
    sums = [down(jnp.sum, row * scale) for row, scale in zip(rows[4:8], scales)]
    masses = [down(jnp.sum, row * scale) for row, scale in zip(rows[8:11], scales[1:])]
    return [*tops, *sums, *masses, down(jnp.sum, rows[11])]


def merge_kernel(stats_ref, out_ref):
    write_copies(jnp.concatenate(combined(stats_ref), axis=0), out_ref)


def finish_kernel(stats_ref, scores_ref, flags_ref, targets_ref, prob_ref, entropy_ref):
    rows = combined(stats_ref)
    scores, flags, targets = scores_ref[...], flags_ref[...], targets_ref[...]
    top = jnp.maximum(rows[0], jnp.max(scores, axis=0, keepdims=True))
    total = rows[4] * jnp.exp(rows[0] - top) + jnp.sum(
        jnp.exp(scores - top), axis=0, keepdims=True
    )
    head_lse = top + jnp.log(total)
    picked = rows[11]
    for k in range(3):
        lse = rows[1 + k] + jnp.log(rows[5 + k])
        mean = rows[8 + k] / rows[5 + k]
        entropy_ref[k : k + 1, :] = flags[k : k + 1].astype(jnp.float32) * (lse - mean)
        low = V_HEAD + k * TAIL
        inside = jnp.logical_and(targets >= low, targets < low + TAIL)
        picked = picked + jnp.where(inside, scores[k : k + 1] - lse, 0.0)
    prob_ref[...] = picked - head_lse


class Heights:
    def __init__(self, count, one, two, three, head, half):
        self.count, self.one, self.two, self.three = count, one, two, three
        self.head, self.half = head, half
        self.three_at = 2 * (one + two)
        self.head_at = 2 * (one + two + three)
        self.rest = 128


def one_device(
    hidden,
    head_weight,
    cluster_weight,
    proj_one,
    proj_two,
    proj_three,
    tail_one,
    tail_two,
    tail_three,
    targets,
    flags,
):
    rows = hidden.shape[0]
    head_cols = head_weight.shape[1]
    tail_cols = tail_one.shape[1]
    half = tail_cols // 2
    n_chips = lax.psum(1, CHIPS)
    n_grp = lax.axis_size("grp")
    core = lax.axis_index(CORE)
    vocab_index = lax.axis_index(VOCAB)

    tails = (tail_one, tail_two, tail_three)
    h = Heights(n_grp, *(t.shape[0] for t in tails), head_weight.shape[0], half)
    shard, other = packed_rows(tails, head_weight, half, h.rest)
    found, others, first, second, owners = ring(shard, other, "grp")

    widths = (proj_one.shape[1], proj_two.shape[1], proj_three.shape[1])
    total = sum(widths)
    share = -(-total // (2 * n_chips) // 8) * 8
    joined = lax.all_gather(
        jnp.concatenate((proj_one, proj_two, proj_three), axis=1), CORE, axis=0, tiled=True
    )
    turned = jnp.pad(joined.T, ((0, 2 * n_chips * share - total), (0, 0)))
    turned = turned.reshape(2, n_chips, share, joined.shape[0])
    pieces = lax.dynamic_index_in_dim(turned, core, 0, keepdims=False)
    pieces = lax.all_to_all(pieces, CHIPS, split_axis=0, concat_axis=0, tiled=True)
    mine = kernel_call(
        project_kernel,
        jax.ShapeDtypeStruct((share, rows), jnp.bfloat16),
        2 * share * hidden.size,
    )(None, pieces, hidden)
    turned = copy_for_each(mine, CHIPS)
    turned = lax.all_gather(turned, CORE)
    turned = turned.reshape(2 * n_chips * share, rows)

    wide = jnp.bfloat16
    part_call = kernel_call(
        functools.partial(part_kernel, h),
        (
            jax.ShapeDtypeStruct((rows, turned.shape[0]), wide),
            jax.ShapeDtypeStruct((rows, head_cols), jnp.float32),
            jax.ShapeDtypeStruct((rows, tail_cols), jnp.float32),
            jax.ShapeDtypeStruct((2, h.two * n_grp, half), wide),
            jax.ShapeDtypeStruct((2, h.three * n_grp, half), wide),
        ),
        2 * rows * (shard.size + other.size) * n_grp,
        [pltpu.VMEM((2, h.one * n_grp, half), wide)],
        mib=16,
    )
    part = part_call(owners, turned, hidden, shard, *found, other, *others)

    cluster_logits = dot(hidden, cluster_weight)
    relative = targets - V_HEAD
    cluster = relative // TAIL
    word = relative - cluster * TAIL
    ids = jnp.stack(
        [targets - vocab_index * head_cols]
        + [jnp.where(cluster == k, word - vocab_index * tail_cols, -1) for k in range(3)],
        axis=1,
    )
    near = VOCAB[1:]
    n_near = lax.psum(1, near)
    n_far = lax.axis_size(VOCAB[0])
    tails_call = kernel_call(
        functools.partial(tails_kernel, h),
        (
            jax.ShapeDtypeStruct((rows, 128), jnp.float32),
            jax.ShapeDtypeStruct((rows, head_cols), jnp.float32),
        ),
        2 * rows * shard.size,
        [pltpu.VMEM((2, h.two * n_grp, half), wide)],
    )
    proj, head_part, *tail_parts = part
    table, head_part = tails_call(owners, first, hidden, proj, head_part, *tail_parts, ids)
    stats = kernel_call(
        functools.partial(last_kernel, h),
        jax.ShapeDtypeStruct((n_near, 1, 12 * rows), jnp.float32),
        2 * rows * other.size,
        mib=8,
    )(owners, second, hidden, head_part, table, ids)
    stats = lax.all_to_all(stats, near, split_axis=0, concat_axis=0, tiled=True)
    stats = kernel_call(
        merge_kernel, jax.ShapeDtypeStruct((n_far, 1, 12 * rows), jnp.float32), 1 << 20, mib=4
    )(None, stats)
    stats = lax.all_to_all(stats, VOCAB[0], split_axis=0, concat_axis=0, tiled=True)
    target_logprob, entropy = kernel_call(
        finish_kernel,
        (
            jax.ShapeDtypeStruct((1, rows), jnp.float32),
            jax.ShapeDtypeStruct((3, rows), jnp.float32),
        ),
        1 << 20,
        mib=4,
    )(None, stats, cluster_logits.T, flags.T, targets[None])
    return (target_logprob[0], entropy.T)


def solution(mesh):
    finer = Mesh(
        mesh.devices.reshape(8, 4, 2, mesh.shape["grp"]), ("vocab_0", "vocab_1", "vocab_2", "grp")
    )
    in_specs = (
        P("grp", None),
        P("grp", VOCAB),
        P(),
        P(VOCAB, None),
        P(VOCAB, None),
        P(VOCAB, None),
        P("grp", VOCAB),
        P("grp", VOCAB),
        P("grp", VOCAB),
        P("grp"),
        P("grp", None),
    )
    out_specs = (P("grp"), P("grp", None))
    return jax.shard_map(
        one_device, mesh=finer, in_specs=in_specs, out_specs=out_specs, check_vma=False
    )
```
